32 devices in a mesh: gx: 4 (over y, core), gy: 8 (over z, x).
Axes of the slice: x: 2, y: 2, z: 4, core: 2. Of those that a mesh axis runs over, the one named last changes fastest.
Arguments:
- tokens: bfloat16 [4, 256, 6144], P('gx', None, 'gy'), may hold values from -6 to 6
- norm_gain: float32 [6144], replicated, may hold values from 0.1 to 1.9
- qkv_weight: bfloat16 [6144, 3, 4096], P('gx', None, 'gy'), may hold values from -0.078125 to 0.078125
- up_weight: bfloat16 [6144, 24576], P('gx', 'gy'), may hold values from -0.078125 to 0.078125
- query_gain: float32 [128], replicated, may hold values from 0.1 to 1.9
- key_gain: float32 [128], replicated, may hold values from 0.1 to 1.9
- out_weight: bfloat16 [4096, 6144], P('gy', 'gx'), may hold values from -0.09375 to 0.09375
- down_weight: bfloat16 [24576, 6144], P('gy', 'gx'), may hold values from -0.0390625 to 0.0390625
- attention_keep: int32 [4, 256, 6144], P('gx', None, 'gy'), may hold values 0 or 1
- feedforward_keep: int32 [4, 256, 6144], P('gx', None, 'gy'), may hold values 0 or 1
Outputs:
- block_out: bfloat16 [4, 256, 6144], P('gx', None, 'gy')
The draws below stay inside these ranges and needn't reach their ends.
All inputs are finite; a program needn't handle non-finite values. No bound on the sum of `attention_keep` or of `feedforward_keep` on one device may be relied on, other than what follows from the above.
Results may differ from the reference program's by a relative error of at most 0.017.
Values may be sent and summed in bfloat16 or wider, within the bound.
No kernel may reach another device: no remote copies, remote signals or barrier semaphores. Data moves between devices by JAX's collectives and lax.ppermute only.
A program may use at most 128 MiB of HBM per device.

```python
import jax
import jax.numpy as jnp
from jax import lax

D = 6144
HEADS = 32
HDIM = 128
FF = 24576
SEQ = 256
IMAGES = 4
INNER = 4096
N_GX = 4
N_GY = 8


def place_ends(entries, key, low, top_value):
    longest = entries.shape.index(max(entries.shape))
    spots = []
    for shift in (0, 1):
        where = [jax.random.randint(jax.random.fold_in(key, axis), (), 0, length) for axis, length in enumerate(entries.shape)]
        where[longest] = (where[longest] + shift) % entries.shape[longest]
        spots.append(tuple(where))
    return entries.at[spots[0]].set(low).at[spots[1]].set(top_value)


def steps_of(stream_key, dims, split, low, largest):
    level, own = 1.0, jax.random.fold_in(stream_key, 6)
    for dim, shards_of in split:
        steps = jnp.exp(jax.random.uniform(jax.random.fold_in(own, dim), (shards_of,), jnp.float32, low / len(split), largest / len(split)))
        level = level * jnp.repeat(steps, dims[dim] // shards_of).reshape([-1 if axis == dim else 1 for axis in range(len(dims))])
    return level


def scatter_about(rng, extent, spread, limit, cuts=(), kind=jnp.bfloat16):
    values = spread * jax.random.normal(rng, extent, jnp.float32)
    if cuts:
        values = values * steps_of(rng, extent, cuts, -0.22, 0.18)
    return jnp.clip(values, -limit, limit).astype(kind)


def setup_inputs(seed: int = 0) -> dict:
    key_of = jax.random.split(jax.random.key(seed), 11)
    return {
        "tokens": scatter_about(key_of[0], (IMAGES, SEQ, D), 1.0, 6.0, ((0, 4), (2, 8))),
        "norm_gain": jnp.clip(1.0 + 0.18 * jax.random.normal(key_of[1], (D,), jnp.float32), 0.1, 1.9),
        "qkv_weight": scatter_about(key_of[2], (D, 3, INNER), D ** -0.5, 0.078125, ((0, 4), (2, 8))),
        "up_weight": scatter_about(key_of[3], (D, FF), D ** -0.5, 0.078125, ((0, 4), (1, 8))),
        "query_gain": jnp.clip(1.0 + 0.18 * jax.random.normal(key_of[4], (HDIM,), jnp.float32), 0.1, 1.9),
        "key_gain": jnp.clip(1.0 + 0.18 * jax.random.normal(key_of[5], (HDIM,), jnp.float32), 0.1, 1.9),
        "out_weight": scatter_about(key_of[6], (INNER, D), INNER ** -0.5, 0.09375, ((0, 8), (1, 4))),
        "down_weight": scatter_about(key_of[7], (FF, D), FF ** -0.5, 0.0390625, ((0, 8), (1, 4))),
        "attention_keep": place_ends((jax.random.randint(key_of[8], (IMAGES, SEQ, D), 0, 10) < 9).astype(jnp.int32), jax.random.fold_in(key_of[8], 1), 0, 1),
        "feedforward_keep": place_ends((jax.random.randint(key_of[9], (IMAGES, SEQ, D), 0, 10) < 9).astype(jnp.int32), jax.random.fold_in(key_of[9], 1), 0, 1),
    }


epsilon = 1e-06
keep_scale = 1.0 / 0.9

def layer_norm(values, gain):
    center = values - lax.optimization_barrier(jnp.mean(values, axis=-1, keepdims=True))
    variance = lax.optimization_barrier(jnp.mean(center * center, axis=-1, keepdims=True))
    return center * lax.rsqrt(variance + epsilon) * gain

def head_norm(values, gain):
    row_count = values.shape[0]
    shaped = values.reshape(row_count, -1, gain.shape[0])
    return layer_norm(shaped, gain).reshape(row_count, -1)

def rounded_sum(left, right, block_width, count):

    def accumulate(running, index):
        offset = index * block_width
        segment = lax.dynamic_slice_in_dim(left, offset, block_width, 1)
        rows_part = lax.dynamic_slice_in_dim(right, offset, block_width, 0)
        term = jnp.dot(segment, rows_part, preferred_element_type=jnp.float32).astype(jnp.bfloat16)
        term = lax.optimization_barrier(term)
        return (running + term.astype(jnp.float32), None)
    begin = jnp.zeros((left.shape[0], right.shape[1]), jnp.float32)
    total, unused = lax.scan(accumulate, begin, jnp.arange(count, dtype=jnp.int32))
    return total

def reference(tokens, norm_gain, qkv_weight, up_weight, query_gain, key_gain, out_weight, down_weight, attention_keep, feedforward_keep):
    row_total = IMAGES * SEQ
    inner = HEADS * HDIM
    normed = layer_norm(tokens.astype(jnp.float32), norm_gain).astype(jnp.bfloat16).reshape(row_total, D)
    joined = jnp.concatenate([qkv_weight.reshape(D, 3 * inner), up_weight], axis=1)
    united = rounded_sum(normed, joined, D // N_GX, N_GX)
    queries = head_norm(united[:, :inner], query_gain).astype(jnp.bfloat16)
    keys = head_norm(united[:, inner:2 * inner], key_gain).astype(jnp.bfloat16)
    values = united[:, 2 * inner:3 * inner].astype(jnp.bfloat16)
    query_grid = queries.reshape(IMAGES, SEQ, HEADS, HDIM).astype(jnp.float32)
    key_grid = keys.reshape(IMAGES, SEQ, HEADS, HDIM).astype(jnp.float32)
    value_grid = values.reshape(IMAGES, SEQ, HEADS, HDIM).astype(jnp.float32)
    scores = jnp.einsum('bshd,bthd->bhst', query_grid, key_grid) * HDIM ** (-0.5)
    raised = jnp.exp(scores)
    weights = (raised / lax.optimization_barrier(jnp.sum(raised, axis=-1, keepdims=True))).astype(jnp.bfloat16)
    attended = jnp.einsum('bhst,bthd->bshd', weights.astype(jnp.float32), value_grid)
    attended = attended.astype(jnp.bfloat16).reshape(row_total, inner)
    hidden = jax.nn.gelu(united[:, 3 * inner:], approximate=False).astype(jnp.bfloat16)
    attention_out = rounded_sum(attended, out_weight, inner // N_GY, N_GY).reshape(IMAGES, SEQ, D)
    feedforward_out = rounded_sum(hidden, down_weight, FF // N_GY, N_GY).reshape(IMAGES, SEQ, D)
    branches = attention_keep.astype(jnp.float32) * attention_out + feedforward_keep.astype(jnp.float32) * feedforward_out
    return (tokens.astype(jnp.float32) + branches * keep_scale).astype(jnp.bfloat16)
```

```python
import jax
import jax.numpy as jnp
from jax import lax
from jax.sharding import PartitionSpec as P

epsilon = 1e-06
keep_scale = 1.0 / 0.9
f32 = jnp.float32
bf16 = jnp.bfloat16


gather_chunks = 2
hidden_chunks = 2


def head_norm(values, gain):
    row_count = values.shape[0]
    shaped = values.reshape(row_count, -1, gain.shape[0])
    center = shaped - jnp.mean(shaped, axis=-1, keepdims=True)
    variance = jnp.mean(center * center, axis=-1, keepdims=True)
    return (center * lax.rsqrt(variance + epsilon) * gain).reshape(row_count, -1)


def bits_of(count):
    return count.bit_length() - 1


def make_per_device(n_gx, n_gy):
    slices = n_gy // n_gx
    low_bits = [1 << b for b in range(bits_of(n_gx))]
    order = [0]
    for bit in reversed(low_bits):
        order = order + [entry ^ bit for entry in order]

    def swap_gx(value, bit):
        return lax.ppermute(value, "gx", [(i, i ^ bit) for i in range(n_gx)])

    def swap_gy(value, bit):
        return lax.ppermute(value, "gy", [(i, i ^ bit) for i in range(n_gy)])

    outward = []
    for g in range(n_gx):
        for block in range(n_gx):
            for s in range(slices):
                place = order.index(g ^ block)
                outward.append((g * n_gy + block * slices + s, block * n_gy + place * slices + s))
    homeward = [(b, a) for a, b in outward]

    def token_stats(tokens):
        values = tokens.astype(f32)
        count = values.shape[-1]
        mean = jnp.mean(values, axis=-1)
        spread = jnp.sum(jnp.square(values - mean[..., None]), axis=-1)
        both = jnp.stack([mean, spread])
        for b in range(bits_of(n_gy)):
            other = swap_gy(both, 1 << b)
            delta = other[0] - both[0]
            both = jnp.stack(
                [0.5 * (both[0] + other[0]), both[1] + other[1] + delta * delta * (0.5 * count)]
            )
            count = 2 * count
        both = jnp.stack([both[0], lax.rsqrt(both[1] / count + epsilon)])[None]
        for bit in reversed(low_bits):
            both = jnp.concatenate([both, swap_gx(both, bit)], axis=0)
        return both

    def sum_over_gx(parts):
        for bit in low_bits:
            half = parts.shape[0] // 2
            moved = swap_gx(parts[half:], bit)
            total = parts[:half].astype(f32) + moved.astype(f32)
            parts = total if half == 1 else total.astype(bf16)
        return parts[0]

    def gather_over_gx(own):
        pieces = [own]
        for bit in reversed(low_bits):
            pieces = pieces + [swap_gx(piece, bit) for piece in pieces]
        return jnp.concatenate(pieces, axis=0)

    def to_owner(part, width):
        rows = part.shape[0] // n_gx
        if slices == 2:
            low = part[:, :width]
            high = part[:, width:]
            upper = lax.axis_index("gy") % 2 == 1
            moved = swap_gy(jnp.where(upper, low, high), 1)
            kept = jnp.where(upper, high, low)
            local = (kept.astype(f32) + moved.astype(f32)).astype(bf16)
        elif slices > 1:
            groups = [[z * slices + s for s in range(slices)] for z in range(n_gx)]
            shaped = part.reshape(n_gx * rows, slices, width).transpose(1, 0, 2)
            local = lax.psum_scatter(
                shaped, "gy", scatter_dimension=0, axis_index_groups=groups, tiled=True
            )
        else:
            local = part
        groups = [[z * slices + s for z in range(n_gx)] for s in range(slices)]
        local = lax.psum_scatter(
            local.reshape(n_gx * rows, width),
            "gy",
            scatter_dimension=0,
            axis_index_groups=groups,
            tiled=True,
        )
        return lax.ppermute(local, ("gx", "gy"), homeward)

    def per_device(
        tokens,
        norm_gain,
        qkv_weight,
        up_weight,
        query_gain,
        key_gain,
        out_weight,
        down_weight,
        attention_keep,
        feedforward_keep,
    ):
        images, seq_len, width = tokens.shape
        block_width = slices * width
        head_cols = qkv_weight.shape[2]
        head_size = query_gain.shape[0]
        own_rows = images * seq_len
        stats = token_stats(tokens)
        gain = lax.dynamic_slice_in_dim(
            norm_gain, lax.axis_index("gx") * block_width, block_width, 0
        )
        chunk = seq_len // gather_chunks
        normed = []
        sent = [
            lax.ppermute(tokens[:, k * chunk : (k + 1) * chunk], ("gx", "gy"), outward)
            for k in range(gather_chunks)
        ]
        for k in range(gather_chunks):
            spread = lax.all_gather(sent[k], "gy", axis=0, tiled=False)
            spread = spread.reshape(n_gx, slices, images, chunk, width)
            spread = spread.transpose(0, 2, 3, 1, 4).reshape(n_gx, images, chunk, block_width)
            part = stats[:, :, :, k * chunk : (k + 1) * chunk]
            mean = part[:, 0][..., None]
            scale = part[:, 1][..., None]
            normed.append(((spread.astype(f32) - mean) * scale * gain).astype(bf16))

        hidden_outs = []
        sub = chunk // hidden_chunks

        def feed_forward(k):
            outs = []
            for h in range(hidden_chunks):
                rows = normed[k][:, :, h * sub : (h + 1) * sub].reshape(-1, block_width)
                parts = jnp.dot(rows, up_weight, preferred_element_type=f32).astype(bf16)
                united = sum_over_gx(parts.reshape(n_gx, images * sub, -1))
                hidden = jax.nn.gelu(united, approximate=False).astype(bf16)
                everyone = gather_over_gx(hidden)
                part = jnp.dot(everyone, down_weight, preferred_element_type=f32).astype(bf16)
                outs.append(to_owner(part, width).reshape(images, sub, width))
            return outs

        qkv_parts = []
        for k in range(gather_chunks):
            rows = normed[k].reshape(-1, block_width)
            products = [
                jnp.dot(rows, qkv_weight[:, j], preferred_element_type=f32).astype(bf16)
                for j in range(3)
            ]
            parts = jnp.concatenate(products, axis=1).reshape(n_gx, images * chunk, -1)
            united = sum_over_gx(parts)
            qkv_parts.append(united.reshape(images, chunk, -1))
            hidden_outs.extend(feed_forward(k))
        united = jnp.concatenate(qkv_parts, axis=1).reshape(own_rows, -1)

        queries = head_norm(united[:, :head_cols], query_gain).astype(bf16)
        keys = head_norm(united[:, head_cols : 2 * head_cols], key_gain).astype(bf16)
        values = united[:, 2 * head_cols : 3 * head_cols].astype(bf16)
        query_grid = queries.reshape(images, seq_len, -1, head_size)
        key_grid = keys.reshape(images, seq_len, -1, head_size)
        value_grid = values.reshape(images, seq_len, -1, head_size)
        scores = jnp.einsum(
            "bshd,bthd->bhst", query_grid, key_grid, preferred_element_type=f32
        ) * head_size ** (-0.5)
        raised = jnp.exp(scores)
        weights = (raised / jnp.sum(raised, axis=-1, keepdims=True)).astype(bf16)
        attended = jnp.einsum("bhst,bthd->bshd", weights, value_grid, preferred_element_type=f32)
        attended = attended.astype(bf16).reshape(own_rows, head_cols)
        attention_part = jnp.dot(
            gather_over_gx(attended), out_weight, preferred_element_type=f32
        ).astype(bf16)
        attention_out = to_owner(attention_part, width).reshape(images, seq_len, width)
        feedforward_out = jnp.concatenate(hidden_outs, axis=1)
        branches = attention_keep.astype(f32) * attention_out.astype(
            f32
        ) + feedforward_keep.astype(f32) * feedforward_out.astype(f32)
        return (tokens.astype(f32) + branches * keep_scale).astype(bf16)

    return per_device


def solution(mesh):
    in_specs = (
        P("gx", None, "gy"),
        P(),
        P("gx", None, "gy"),
        P("gx", "gy"),
        P(),
        P(),
        P("gy", "gx"),
        P("gy", "gx"),
        P("gx", None, "gy"),
        P("gx", None, "gy"),
    )
    out_specs = P("gx", None, "gy")
    return jax.shard_map(
        make_per_device(mesh.shape["gx"], mesh.shape["gy"]),
        mesh=mesh,
        in_specs=in_specs,
        out_specs=out_specs,
        check_vma=False,
    )
```
